32 devices in a mesh: dap: 8 (over z, x), cplx: 4 (over y, core).
Axes of the slice: x: 2, y: 2, z: 4, core: 2. Of those that a mesh axis runs over, the one named last changes fastest.
Arguments:
- pair: bfloat16 [96, 384, 128], P('dap', 'cplx'), parts along dimension 1, may hold values from -6 to 6
- cotangent: bfloat16 [96, 384, 128], P('dap', 'cplx'), parts along dimension 1, may hold values from -6 to 6
- residue_mask: int32 [384], P('cplx'), parts along dimension 0, may hold values 0 or 1
- chain_ids: int32 [384], P('cplx'), parts along dimension 0, may hold values from 0 to 2, never falling along the last dimension, each value on 1 to 48 neighbouring positions
- chain_embed: float32 [2, 128], replicated, may hold values from -4 to 4
- out_norm_gain: float32 [128], replicated, may hold values from 0.25 to 1.75
- out_proj: bfloat16 [128, 512], replicated, may hold values from -0.5 to 0.5
- out_gate: bfloat16 [128, 128], replicated, may hold values from -0.5 to 0.5
- out_mid_gain: float32 [128], replicated, may hold values from 0.25 to 1.75
- out_final: bfloat16 [128, 128], replicated, may hold values from -0.5 to 0.5
- in_norm_gain: float32 [128], replicated, may hold values from 0.25 to 1.75
- in_proj: bfloat16 [128, 512], replicated, may hold values from -0.5 to 0.5
- in_gate: bfloat16 [128, 128], replicated, may hold values from -0.5 to 0.5
- in_mid_gain: float32 [128], replicated, may hold values from 0.25 to 1.75
- in_final: bfloat16 [128, 128], replicated, may hold values from -0.5 to 0.5
Outputs:
- pair_grad: bfloat16 [96, 384, 128], P('dap', 'cplx'), parts along dimension 1
- grad_proj: float32 [512, 512], P('cplx'), parts along dimension 0
- grad_gate: float32 [512, 128], P('cplx'), parts along dimension 0
- grad_final: float32 [512, 128], P('cplx'), parts along dimension 0
- grad_norm_gain: float32 [512], P('cplx'), parts along dimension 0
- grad_mid_gain: float32 [512], P('cplx'), parts along dimension 0
The draws below stay inside these ranges and needn't reach their ends.
There are 4 independent parts, one for each index of `cplx`. The reference program is written for one: setup_inputs(seed, part) draws one part's arguments, and reference() takes and returns one part's arrays. A program takes and returns all parts, laid end to end along the dimension named above; an argument that names none is the same for every part. Nothing has to cross between parts.
Inputs may be any that keep to these rules, and one draw needn't show every extreme that they name: `chain_ids`: chain numbers never fall along the residues; each chain has at most 48 residues.
All inputs are finite; a program needn't handle non-finite values.
Results may differ from the reference program's by a relative error of at most 0.019.
Values may be sent and summed in bfloat16 or wider, within the bound.
A program may use at most 128 MiB of HBM per device.

```python
import math
import jax
import jax.numpy as jnp
import numpy as np
from jax import lax

C = 128
HID = 128
N_RES = 96


def plant(result, rng, smallest, high):
    place = [jax.random.randint(jax.random.fold_in(rng, axis), (), 0, length) for axis, length in enumerate(result.shape)]
    widest = result.shape.index(max(result.shape))
    neighbour = place[:widest] + [(place[widest] + 1) % result.shape[widest]] + place[widest + 1:]
    return result.at[tuple(place)].set(smallest).at[tuple(neighbour)].set(high)


def shard_levels(key, extent, cuts, least, high):
    factor_of = 1.0
    for position, blocks in cuts:
        draws = jax.random.uniform(jax.random.fold_in(jax.random.fold_in(key, 6), position), (blocks,), jnp.float32, least / len(cuts), high / len(cuts))
        factor_of = factor_of * jnp.repeat(jnp.exp(draws), extent[position] // blocks).reshape((-1,) + (1,) * (len(extent) - 1 - position))
    return factor_of


def split_up(number_of, total, most, skew):
    loads = [(1 << 20) // math.isqrt(rank ** skew) + 1 for rank in range(2, number_of + 1)]
    surplus, counts = total - most - (number_of - 1), [1] * (number_of - 1)
    while surplus > 0:
        free = [i for i in range(number_of - 1) if counts[i] < most]
        pool, left = sum([loads[i] for i in free]), surplus
        for i in free:
            addition = min(most - counts[i], max(1, left * loads[i] // pool), surplus)
            counts[i] = counts[i] + addition
            surplus = surplus - addition
    return np.array([most] + counts)


def uneven_parts(rng, amount, total, limit, skew):
    if amount == 2:
        one = jax.random.randint(rng, (), max(1, total - limit), min(limit, total - 1) + 1)
        return jnp.stack([one, total - one])
    tallies = jnp.asarray(split_up(amount, total, limit, skew), jnp.int32)
    twos = (amount - 1) // 2
    donor, sink = tallies[1:1 + 2 * twos:2], tallies[2:2 + 2 * twos:2]
    margin = jnp.minimum(donor - 1, limit - sink)
    shifted = jax.random.randint(jax.random.fold_in(rng, 1), (twos,), 0, 1 << 20) % (margin + 1)
    tallies = tallies.at[1:1 + 2 * twos:2].set(donor - shifted).at[2:2 + 2 * twos:2].set(sink + shifted)
    return tallies[jax.random.permutation(jax.random.fold_in(rng, 2), amount)]


def normal_values(stream_key, dims, deviation, most, cuts=(), dtype=jnp.bfloat16):
    drawn = jax.random.normal(stream_key, dims, jnp.float32) * deviation
    if len(cuts) > 0:
        drawn = shard_levels(stream_key, dims, cuts, -0.22, 0.18) * drawn
    return jnp.clip(drawn, min=-most, max=most).astype(dtype)


def setup_inputs(seed: int = 0, part: int = 0) -> dict:
    arg_keys = jax.random.split(jax.random.key(seed), 16)
    part_splits = jax.random.split(jax.random.fold_in(arg_keys[15], part), 16)
    return {
        "pair": normal_values(part_splits[0], (N_RES, N_RES, C), 1.0, 6.0, ((0, 8),)),
        "cotangent": normal_values(part_splits[1], (N_RES, N_RES, C), 1.0, 6.0, ((0, 8),)),
        "residue_mask": plant((jax.random.randint(part_splits[2], (N_RES,), 0, 8) < 7).astype(jnp.int32), jax.random.fold_in(part_splits[2], 1), 0, 1),
        "chain_ids": jnp.searchsorted(jnp.cumsum(uneven_parts(part_splits[3], 3, N_RES, N_RES // 2, 0)), jnp.arange(N_RES), side="right").astype(jnp.int32),
        "chain_embed": normal_values(arg_keys[4], (2, C), 1.0, 4.0, (), jnp.float32),
        "out_norm_gain": jnp.clip(1.0 + 0.15 * jax.random.normal(arg_keys[5], (C,), jnp.float32), 0.25, 1.75),
        "out_proj": normal_values(arg_keys[6], (C, 4 * HID), C ** -0.5, 0.5),
        "out_gate": normal_values(arg_keys[7], (C, C), C ** -0.5, 0.5),
        "out_mid_gain": jnp.clip(1.0 + 0.15 * jax.random.normal(arg_keys[8], (HID,), jnp.float32), 0.25, 1.75),
        "out_final": normal_values(arg_keys[9], (HID, C), HID ** -0.5, 0.5),
        "in_norm_gain": jnp.clip(1.0 + 0.15 * jax.random.normal(arg_keys[10], (C,), jnp.float32), 0.25, 1.75),
        "in_proj": normal_values(arg_keys[11], (C, 4 * HID), C ** -0.5, 0.5),
        "in_gate": normal_values(arg_keys[12], (C, C), C ** -0.5, 0.5),
        "in_mid_gain": jnp.clip(1.0 + 0.15 * jax.random.normal(arg_keys[13], (HID,), jnp.float32), 0.25, 1.75),
        "in_final": normal_values(arg_keys[14], (HID, C), HID ** -0.5, 0.5),
    }


def layer_norm(values_in, gain):
    average = lax.optimization_barrier(jnp.mean(values_in, axis=-1, keepdims=True))
    centred = values_in - average
    variance = lax.optimization_barrier(jnp.mean(centred * centred, axis=-1, keepdims=True))
    return centred * jax.lax.rsqrt(variance + 1e-05) * gain

def gated_pair(projected, pair_mask, hidden_width):
    masked = pair_mask[..., None]
    left_act = masked * jax.nn.sigmoid(projected[..., :hidden_width]) * projected[..., hidden_width:2 * hidden_width]
    right_act = masked * jax.nn.sigmoid(projected[..., 2 * hidden_width:3 * hidden_width]) * projected[..., 3 * hidden_width:]
    return (left_act, right_act)

def reference(pair, cotangent, residue_mask, chain_ids, chain_embed, out_norm_gain, out_proj, out_gate, out_mid_gain, out_final, in_norm_gain, in_proj, in_gate, in_mid_gain, in_final):
    f32 = jnp.float32
    bf16 = jnp.bfloat16
    hidden_width = out_final.shape[0]
    res_count = pair.shape[0]
    inv_count = 1.0 / res_count
    pair_mask = (residue_mask[:, None] * residue_mask[None, :]).astype(f32)
    same_chain = chain_ids[:, None] == chain_ids[None, :]
    start = pair.astype(f32) + jnp.where(same_chain[..., None], chain_embed[1], chain_embed[0])
    out_normed = layer_norm(start, out_norm_gain).astype(bf16)
    projected = jnp.dot(out_normed, out_proj, preferred_element_type=f32)
    left_act, right_act = gated_pair(projected, pair_mask, hidden_width)
    left_b = left_act.astype(bf16)
    right_b = right_act.astype(bf16)
    x_out = jnp.einsum('ikc,jkc->ijc', left_b.astype(f32), right_b.astype(f32))
    y_out = layer_norm(x_out, out_mid_gain).astype(bf16)
    update = jax.nn.sigmoid(jnp.dot(out_normed, out_gate, preferred_element_type=f32)) * jnp.dot(y_out, out_final, preferred_element_type=f32)
    pair_mid = (start + update).astype(bf16)
    mid_f32 = pair_mid.astype(f32)
    normed_f32, norm_back = jax.vjp(layer_norm, mid_f32, in_norm_gain)
    in_normed = normed_f32.astype(bf16)
    proj_in = jnp.dot(in_normed, in_proj, preferred_element_type=f32)
    (left_in, right_in), glu_back = jax.vjp(lambda proj_val: gated_pair(proj_val, pair_mask, hidden_width), proj_in)
    left_ib = left_in.astype(bf16)
    right_ib = right_in.astype(bf16)
    x_in = jnp.einsum('kic,kjc->ijc', left_ib.astype(f32), right_ib.astype(f32))
    y_f32, mid_back = jax.vjp(layer_norm, x_in, in_mid_gain)
    y_in = y_f32.astype(bf16)
    logit = jnp.dot(in_normed, in_gate, preferred_element_type=f32)
    value = jnp.dot(y_in, in_final, preferred_element_type=f32)
    sigma = jax.nn.sigmoid(logit)
    upstream = cotangent.astype(f32)
    grad_value = (upstream * sigma).astype(bf16)
    grad_logit = (upstream * value * sigma * (1.0 - sigma)).astype(bf16)
    grad_final = jnp.einsum('ijc,ijd->cd', y_in.astype(f32), grad_value.astype(f32)) * inv_count
    grad_gate = jnp.einsum('ijc,ijd->cd', in_normed.astype(f32), grad_logit.astype(f32)) * inv_count
    grad_y = jnp.dot(grad_value, in_final.T, preferred_element_type=f32)
    grad_x, grad_mid = mid_back(grad_y)
    grad_x_b = grad_x.astype(bf16).astype(f32)
    grad_a = jnp.einsum('kjc,ijc->kic', right_ib.astype(f32), grad_x_b)
    grad_b = jnp.einsum('kic,ijc->kjc', left_ib.astype(f32), grad_x_b)
    grad_p = glu_back((grad_a, grad_b))[0].astype(bf16)
    grad_proj = jnp.einsum('ijc,ijd->cd', in_normed.astype(f32), grad_p.astype(f32)) * inv_count
    grad_normed = jnp.dot(grad_p, in_proj.T, preferred_element_type=f32) + jnp.dot(grad_logit, in_gate.T, preferred_element_type=f32)
    grad_z, grad_norm = norm_back(grad_normed)
    pair_grad = (upstream + grad_z).astype(bf16)
    return (pair_grad, grad_proj, grad_gate, grad_final, grad_norm * inv_count, grad_mid * inv_count)
```

```python
import functools

import jax
import jax.numpy as jnp
from jax import lax
from jax.experimental import pallas as pl
from jax.experimental.pallas import tpu as pltpu
from jax.sharding import PartitionSpec as P

F32 = jnp.float32
BF16 = jnp.bfloat16
LANES = 128
A_OUT, B_OUT, X_OUT, A_IN, B_IN, X_IN, G_X, G_A, G_B, P_SUM, P_ALL = range(11)


def tn(w, x):
    return lax.dot_general(w, x, (((0,), (0,)), ((), ())), preferred_element_type=F32)


def nn(w, x):
    return jnp.dot(w, x, preferred_element_type=F32)


def nt(w, x):
    return lax.dot_general(w, x, (((1,), (1,)), ((), ())), preferred_element_type=F32)


def sigmoid(v):
    return 1.0 / (1.0 + jnp.exp(-v))


def norm_stats(v):
    centred = v - jnp.mean(v, axis=0, keepdims=True)
    inv = lax.rsqrt(jnp.mean(centred * centred, axis=0, keepdims=True) + 1e-05)
    return centred * inv, inv


def norm_back(grad, hat, inv, gain):
    scaled = grad * gain
    m1 = jnp.mean(scaled, axis=0, keepdims=True)
    m2 = jnp.mean(scaled * hat, axis=0, keepdims=True)
    return inv * (scaled - m1 - hat * m2)


def lane_sum(v):
    return jnp.sum(v, axis=1, keepdims=True)


def kernel(
    n, rows, res, lc,
    pair, cot, masks, params, out_proj, out_gate, out_final, in_proj, in_gate, in_final,
    grad_out, gp_out, gg_out, gf_out, gains_out,
    cols, start, normed, gate, in_p, cot_t, mid, logit_s, gv, gy, gl,
    a_s, b_s, x_s, a_r, b_r, x_r,
    a2_s, b2_s, x2_s, a2_r, b2_r, x2_r,
    gx_s, gx_r, ga_s, gb_s, ga_r, gb_r,
    slab_a, slab_b, slab_o, slab_p, mat_a, mat_b,
    acc_p, acc_g, acc_f, acc_n, acc_m, g_s, g_r, t_s, t_r,
    send_sem, recv_sem,
):
    me = lax.axis_index("dap")
    c = start.shape[0]
    per = c // n
    total = rows * res
    chunks = total // lc
    tiles = -(-res // LANES)
    inv_count = 1.0 / res

    barrier = pltpu.get_barrier_semaphore()
    for p in range(1, n):
        pl.semaphore_signal(
            barrier, inc=1, device_id={"dap": lax.rem(me + p, n)},
            device_id_type=pl.DeviceIdType.MESH,
        )
    pl.semaphore_wait(barrier, n - 1)

    def copy_to(which, src, dst, peer):
        return pltpu.make_async_remote_copy(
            src_ref=src, dst_ref=dst,
            send_sem=send_sem.at[which, peer], recv_sem=recv_sem.at[which, me],
            device_id={"dap": peer}, device_id_type=pl.DeviceIdType.MESH,
        )

    def spread(which, src, dst):
        for p in range(1, n):
            peer = lax.rem(me + p, n)
            copy_to(which, src.at[peer], dst.at[me], peer).start()
        dst[me] = src[me]

    def collect(which, src, dst):
        for p in range(1, n):
            peer = lax.rem(me + n - p, n)
            pltpu.make_async_remote_copy(
                src_ref=src.at[peer], dst_ref=dst.at[peer],
                send_sem=send_sem.at[which, peer], recv_sem=recv_sem.at[which, peer],
                device_id={"dap": peer}, device_id_type=pl.DeviceIdType.MESH,
            ).wait()

    def lanes_of(k):
        return pl.ds(pl.multiple_of(k * lc, lc), lc)

    def put(ref, ds, value):
        ref[:, :, ds] = value.reshape(n, per, lc).astype(BF16)

    def take(ref, ds):
        return ref[:, :, ds].astype(F32).reshape(c, lc)

    def to_slab(ref, slab):
        def one(s, _):
            block = ref[s].astype(F32)
            for i in range(rows):
                part = block[:, i * res : (i + 1) * res]
                at = pl.ds(pl.multiple_of((s * rows + i) * per, per), per)
                for t in range(tiles):
                    width = min(LANES, res - t * LANES)
                    slab[t, at, :width] = part[:, t * LANES : t * LANES + width]
            return 0

        lax.fori_loop(0, n, one, 0)

    def matrix(slab, ch):
        parts = [slab[t, pl.ds(ch, res, stride=per), :] for t in range(tiles)]
        whole = parts[0] if tiles == 1 else jnp.concatenate(parts, axis=1)
        return whole[:, :res].astype(BF16)

    def keep(slab, ch, value):
        pad = tiles * LANES - res
        if pad:
            value = jnp.concatenate([value, jnp.zeros((res, pad), F32)], axis=1)
        for t in range(tiles):
            slab[t, pl.ds(ch, res, stride=per), :] = value[:, t * LANES : (t + 1) * LANES]

    def from_slab(slab, ref):
        def one(s, _):
            parts = []
            for i in range(rows):
                at = pl.ds(pl.multiple_of((s * rows + i) * per, per), per)
                for t in range(tiles):
                    width = min(LANES, res - t * LANES)
                    parts.append(slab[t, at, :width])
            ref[s] = jnp.concatenate(parts, axis=1).astype(BF16)
            return 0

        lax.fori_loop(0, n, one, 0)

    cols[...] = params[...].T
    emb0, emb1 = cols[:, 0:1], cols[:, 1:2]
    g_on, g_om, g_in, g_im = (cols[:, q : q + 1] for q in range(2, 6))

    @pl.loop(0, chunks)
    def _(k):
        ds = lanes_of(k)
        same = masks[1:2, ds] > 0.5
        x = pair[ds, :].astype(F32).T + jnp.where(same, emb1, emb0)
        start[:, ds] = x
        hat, _ = norm_stats(x)
        nb = (hat * g_on).astype(BF16)
        normed[:, ds] = nb
        p = tn(out_proj[...], nb)
        pm = masks[0:1, ds]
        put(a_s, ds, pm * sigmoid(p[:c]) * p[c : 2 * c])
        put(b_s, ds, pm * sigmoid(p[2 * c : 3 * c]) * p[3 * c :])

    spread(A_OUT, a_s, a_r)
    spread(B_OUT, b_s, b_r)

    @pl.loop(0, chunks)
    def _(k):
        ds = lanes_of(k)
        gate[:, ds] = sigmoid(tn(out_gate[...], normed[:, ds]))
        cot_t[:, ds] = cot[ds, :].astype(F32).T

    collect(A_OUT, a_s, a_r)
    to_slab(a_r, slab_a)
    collect(B_OUT, b_s, b_r)
    to_slab(b_r, slab_b)
    for ch in range(per):
        keep(slab_o, ch, nt(matrix(slab_a, ch), matrix(slab_b, ch)))
    from_slab(slab_o, x_s)
    spread(X_OUT, x_s, x_r)
    collect(X_OUT, x_s, x_r)

    @pl.loop(0, chunks)
    def _(k):
        ds = lanes_of(k)
        hat, _ = norm_stats(take(x_r, ds))
        y = (hat * g_om).astype(BF16)
        m = (start[:, ds] + gate[:, ds] * tn(out_final[...], y)).astype(BF16)
        mid[:, ds] = m
        hat, _ = norm_stats(m.astype(F32))
        nb = (hat * g_in).astype(BF16)
        normed[:, ds] = nb
        p = tn(in_proj[...], nb)
        in_p[:, ds] = p
        pm = masks[0:1, ds]
        put(a2_s, ds, pm * sigmoid(p[:c]) * p[c : 2 * c])
        put(b2_s, ds, pm * sigmoid(p[2 * c : 3 * c]) * p[3 * c :])

    spread(A_IN, a2_s, a2_r)
    spread(B_IN, b2_s, b2_r)

    @pl.loop(0, chunks)
    def _(k):
        ds = lanes_of(k)
        s = sigmoid(tn(in_gate[...], normed[:, ds]))
        logit_s[:, ds] = s
        v = (cot_t[:, ds] * s).astype(BF16)
        gv[:, ds] = v
        gy[:, ds] = nn(in_final[...], v)

    acc_p[...] = jnp.zeros_like(acc_p)
    acc_g[...] = jnp.zeros_like(acc_g)
    acc_f[...] = jnp.zeros_like(acc_f)
    acc_n[...] = jnp.zeros_like(acc_n)
    acc_m[...] = jnp.zeros_like(acc_m)

    collect(A_IN, a2_s, a2_r)
    to_slab(a2_r, slab_a)
    collect(B_IN, b2_s, b2_r)
    to_slab(b2_r, slab_b)
    for ch in range(per):
        a = matrix(slab_a, ch)
        b = matrix(slab_b, ch)
        mat_a[ch] = a
        mat_b[ch] = b
        keep(slab_o, ch, tn(a, b))
    from_slab(slab_o, x2_s)
    spread(X_IN, x2_s, x2_r)
    collect(X_IN, x2_s, x2_r)

    @pl.loop(0, chunks)
    def _(k):
        ds = lanes_of(k)
        hat, inv = norm_stats(take(x2_r, ds))
        y = (hat * g_im).astype(BF16)
        value = tn(in_final[...], y)
        s = logit_s[:, ds]
        grad_l = (cot_t[:, ds] * value * s * (1.0 - s)).astype(BF16)
        gl[:, ds] = grad_l
        g = gy[:, ds]
        acc_m[...] += lane_sum(g * hat)
        put(gx_s, ds, norm_back(g, hat, inv, g_im))
        acc_f[...] += nt(y, gv[:, ds])

    spread(G_X, gx_s, gx_r)

    @pl.loop(0, chunks)
    def _(k):
        ds = lanes_of(k)
        grad_l = gl[:, ds]
        acc_g[...] += nt(normed[:, ds], grad_l)
        gy[:, ds] = nn(in_gate[...], grad_l)

    collect(G_X, gx_s, gx_r)
    to_slab(gx_r, slab_a)
    for ch in range(per):
        gx = matrix(slab_a, ch)
        keep(slab_o, ch, nt(mat_b[ch], gx))
        keep(slab_p, ch, nn(mat_a[ch], gx))
    from_slab(slab_o, ga_s)
    spread(G_A, ga_s, ga_r)
    from_slab(slab_p, gb_s)
    spread(G_B, gb_s, gb_r)
    collect(G_A, ga_s, ga_r)
    collect(G_B, gb_s, gb_r)

    @pl.loop(0, chunks)
    def _(k):
        ds = lanes_of(k)
        pm = masks[0:1, ds]
        s0 = sigmoid(in_p[:c, ds])
        s2 = sigmoid(in_p[2 * c : 3 * c, ds])
        ga = take(ga_r, ds) * pm * s0
        gb = take(gb_r, ds) * pm * s2
        q0 = (ga * in_p[c : 2 * c, ds] * (1.0 - s0)).astype(BF16)
        q2 = (gb * in_p[3 * c :, ds] * (1.0 - s2)).astype(BF16)
        q = jnp.concatenate([q0, ga.astype(BF16), q2, gb.astype(BF16)], axis=0)
        acc_p[...] += nt(normed[:, ds], q)
        g = nn(in_proj[...], q) + gy[:, ds]
        hat, inv = norm_stats(mid[:, ds].astype(F32))
        acc_n[...] += lane_sum(g * hat)
        z = cot_t[:, ds] + norm_back(g, hat, inv, g_in)
        grad_out[ds, :] = z.T.astype(BF16)

    lane = lax.broadcasted_iota(jnp.int32, (c, LANES), 1)
    gains = jnp.where(lane == 0, acc_n[...], jnp.where(lane == 1, acc_m[...], 0.0))
    whole = jnp.concatenate([acc_p[...], acc_g[...], acc_f[...], gains], axis=1) * inv_count
    g_s[...] = whole.reshape(n, per, whole.shape[1]).astype(BF16)
    spread(P_SUM, g_s, g_r)
    collect(P_SUM, g_s, g_r)
    summed = jnp.sum(g_r[...].astype(F32), axis=0).astype(BF16)
    t_s[...] = summed
    for p in range(1, n):
        peer = lax.rem(me + p, n)
        copy_to(P_ALL, t_s, t_r.at[me], peer).start()
    t_r[me] = summed
    for p in range(1, n):
        peer = lax.rem(me + n - p, n)
        pltpu.make_async_remote_copy(
            src_ref=t_s, dst_ref=t_r.at[peer],
            send_sem=send_sem.at[P_ALL, peer], recv_sem=recv_sem.at[P_ALL, peer],
            device_id={"dap": peer}, device_id_type=pl.DeviceIdType.MESH,
        ).wait()
    final = t_r[...].astype(F32).reshape(c, t_r.shape[2])
    gp_out[...] = final[:, : 4 * c]
    gg_out[...] = final[:, 4 * c : 5 * c]
    gf_out[...] = final[:, 5 * c : 6 * c]
    gains_out[...] = final[:, 6 * c :].T[:8]


def shards(n, pair, cotangent, residue_mask, chain_ids, chain_embed, out_norm_gain, out_proj,
           out_gate, out_mid_gain, out_final, in_norm_gain, in_proj, in_gate, in_mid_gain, in_final):
    rows, res, c = pair.shape
    total = rows * res
    per = c // n
    lc = max(q for q in range(LANES, 3 * LANES + 1, LANES) if total % q == 0)
    tiles = -(-res // LANES)
    row_start = lax.axis_index("dap") * rows
    row_mask = lax.dynamic_slice_in_dim(residue_mask, row_start, rows, 0)
    row_chain = lax.dynamic_slice_in_dim(chain_ids, row_start, rows, 0)
    pair_mask = (row_mask[:, None] * residue_mask[None, :]).astype(F32)
    same = (row_chain[:, None] == chain_ids[None, :]).astype(F32)
    masks = jnp.stack([pair_mask.reshape(total), same.reshape(total)])
    params = jnp.concatenate(
        [chain_embed, jnp.stack([out_norm_gain, out_mid_gain, in_norm_gain, in_mid_gain]),
         jnp.zeros((2, c), F32)], axis=0)

    def full(dtype):
        return pltpu.VMEM((c, total), dtype)

    swap = pltpu.VMEM((n, per, total), BF16)
    slab = pltpu.VMEM((tiles, res * per, LANES), F32)
    mats = pltpu.VMEM((per, res, res), BF16)
    wide = 6 * c + LANES
    scratch = [
        pltpu.VMEM((c, 8), F32), full(F32), full(BF16), full(F32),
        pltpu.VMEM((4 * c, total), F32), full(F32), full(BF16), full(F32), full(BF16), full(F32),
        full(BF16),
    ] + [swap] * 18 + [slab] * 4 + [mats] * 2 + [
        pltpu.VMEM((c, 4 * c), F32), pltpu.VMEM((c, c), F32), pltpu.VMEM((c, c), F32),
        pltpu.VMEM((c, 1), F32), pltpu.VMEM((c, 1), F32),
        pltpu.VMEM((n, per, wide), BF16), pltpu.VMEM((n, per, wide), BF16),
        pltpu.VMEM((per, wide), BF16), pltpu.VMEM((n, per, wide), BF16),
        pltpu.SemaphoreType.DMA((11, n)), pltpu.SemaphoreType.DMA((11, n)),
    ]
    vmem = pl.BlockSpec(memory_space=pltpu.VMEM)
    grad, gp, gg, gf, gains = pl.pallas_call(
        functools.partial(kernel, n, rows, res, lc),
        out_shape=(
            jax.ShapeDtypeStruct((total, c), BF16),
            jax.ShapeDtypeStruct((c, 4 * c), F32),
            jax.ShapeDtypeStruct((c, c), F32),
            jax.ShapeDtypeStruct((c, c), F32),
            jax.ShapeDtypeStruct((8, c), F32),
        ),
        in_specs=[vmem] * 10,
        out_specs=(vmem,) * 5,
        scratch_shapes=scratch,
        compiler_params=pltpu.CompilerParams(
            collective_id=0, has_side_effects=True, vmem_limit_bytes=60 * 1024 * 1024
        ),
    )(
        pair.reshape(total, c), cotangent.reshape(total, c), masks, params,
        out_proj, out_gate, out_final, in_proj, in_gate, in_final,
    )
    return grad.reshape(rows, res, c), gp, gg, gf, gains[0], gains[1]


def solution(mesh):
    split = P("dap", "cplx", None)
    return jax.shard_map(
        functools.partial(shards, mesh.shape["dap"]),
        mesh=mesh,
        in_specs=(split, split, P("cplx"), P("cplx")) + (P(),) * 11,
        out_specs=(split, P("cplx", None), P("cplx", None), P("cplx", None), P("cplx"), P("cplx")),
        check_vma=False,
    )
```

```python
import functools

import jax
import jax.numpy as jnp
from jax import lax
from jax.experimental import pallas as pl
from jax.experimental.pallas import tpu as pltpu
from jax.sharding import PartitionSpec as P

F32 = jnp.float32
BF16 = jnp.bfloat16
LANES = 128
A_OUT, B_OUT, X_OUT, A_IN, B_IN, X_IN, G_X, G_A, G_B, P_SUM, P_ALL, H_SUM, H_ALL = range(13)


def tn(w, x):
    return lax.dot_general(w, x, (((0,), (0,)), ((), ())), preferred_element_type=F32)


def nn(w, x):
    return jnp.dot(w, x, preferred_element_type=F32)


def nt(w, x):
    return lax.dot_general(w, x, (((1,), (1,)), ((), ())), preferred_element_type=F32)


def sigmoid(v):
    return 1.0 / (1.0 + jnp.exp(-v))


def norm_stats(v):
    centred = v - jnp.mean(v, axis=0, keepdims=True)
    inv = lax.rsqrt(jnp.mean(centred * centred, axis=0, keepdims=True) + 1e-05)
    return centred * inv, inv


def norm_back(grad, hat, inv, gain):
    scaled = grad * gain
    m1 = jnp.mean(scaled, axis=0, keepdims=True)
    m2 = jnp.mean(scaled * hat, axis=0, keepdims=True)
    return inv * (scaled - m1 - hat * m2)


def lane_sum(v):
    return jnp.sum(v, axis=1, keepdims=True)


def kernel(
    n, rows, res, lc,
    pair, cot, masks, params, out_proj, out_gate, out_final, in_proj, in_gate, in_final,
    grad_out, gp_out, gg_out, gf_out, gains_out,
    cols, start, normed, gate, in_p, cot_t, mid, logit_s, gv, gy, gl,
    a_s, b_s, x_s, a_r, b_r, x_r,
    a2_s, b2_s, x2_s, a2_r, b2_r, x2_r,
    gx_s, gx_r, ga_s, gb_s, ga_r, gb_r,
    slab_a, slab_b, slab_o, slab_p, mat_a, mat_b,
    acc_p, acc_g, acc_f, acc_n, acc_m, g_s, g_r, t_s, t_r, h_s, h_r, u_s, u_r,
    send_sem, recv_sem,
):
    me = lax.axis_index("dap")
    c = start.shape[0]
    per = c // n
    total = rows * res
    chunks = total // lc
    crows = lc // res
    tiles = -(-res // LANES)
    inv_count = 1.0 / res

    barrier = pltpu.get_barrier_semaphore()
    for p in range(1, n):
        pl.semaphore_signal(
            barrier, inc=1, device_id={"dap": lax.rem(me + p, n)},
            device_id_type=pl.DeviceIdType.MESH,
        )
    pl.semaphore_wait(barrier, n - 1)

    def copy_to(sem, src, dst, peer):
        return pltpu.make_async_remote_copy(
            src_ref=src, dst_ref=dst, send_sem=send_sem.at[sem], recv_sem=recv_sem.at[sem],
            device_id={"dap": peer}, device_id_type=pl.DeviceIdType.MESH,
        )

    def spread(which, src, dst, k=0, ds=None):
        def view(ref, at):
            return ref.at[at] if ds is None else ref.at[at, :, ds]

        for p in range(1, n):
            peer = lax.rem(me + p, n)
            copy_to(which * chunks + k, view(src, peer), view(dst, me), peer).start()
        if ds is None:
            dst[me] = src[me]
        else:
            dst[me, :, ds] = src[me, :, ds]

    def collect(which, src, dst, k=0, ds=None):
        def view(ref):
            return ref.at[pl.ds(0, n - 1)] if ds is None else ref.at[pl.ds(0, n - 1), :, ds]

        copy_to(which * chunks + k, view(src), view(dst), lax.rem(me + 1, n)).wait()

    def lanes_of(k):
        return pl.ds(pl.multiple_of(k * lc, lc), lc)

    def put(ref, ds, value):
        ref[:, :, ds] = value.reshape(n, per, lc).astype(BF16)

    def take(ref, ds):
        return ref[:, :, ds].astype(F32).reshape(c, lc)

    def to_slab(ref, slab, k, by_chunk=False):
        for s in range(n):
            block = ref[s, :, lanes_of(k)].astype(F32)
            row = (k * n + s) * crows if by_chunk else s * rows + k * crows
            for i in range(crows):
                part = block[:, i * res : (i + 1) * res]
                at = pl.ds(pl.multiple_of((row + i) * per, per), per)
                for t in range(tiles):
                    width = min(LANES, res - t * LANES)
                    slab[t, at, :width] = part[:, t * LANES : t * LANES + width]

    def matrix(slab, ch, first=0, count=res):
        at = pl.ds(first * per + ch, count, stride=per)
        parts = [slab[t, at, :] for t in range(tiles)]
        whole = parts[0] if tiles == 1 else jnp.concatenate(parts, axis=1)
        return whole[:, :res].astype(BF16)

    def keep(slab, ch, value, first=0):
        count = value.shape[0]
        pad = tiles * LANES - res
        if pad:
            value = jnp.concatenate([value, jnp.zeros((count, pad), F32)], axis=1)
        for t in range(tiles):
            at = pl.ds(first * per + ch, count, stride=per)
            slab[t, at, :] = value[:, t * LANES : (t + 1) * LANES]

    def from_slab(slab, ref, k, by_chunk=False):
        for s in range(n):
            row = (k * n + s) * crows if by_chunk else s * rows + k * crows
            parts = []
            for i in range(crows):
                at = pl.ds(pl.multiple_of((row + i) * per, per), per)
                for t in range(tiles):
                    width = min(LANES, res - t * LANES)
                    parts.append(slab[t, at, :width])
            ref[s, :, lanes_of(k)] = jnp.concatenate(parts, axis=1).astype(BF16)

    def early():
        return jnp.concatenate([acc_g[...], acc_f[...]], axis=1) * inv_count

    def hand_round(which, src, mine, dst):
        summed = jnp.sum(src[...].astype(F32), axis=0).astype(BF16)
        mine[...] = summed
        for p in range(1, n):
            copy_to(which * chunks, mine, dst.at[me], lax.rem(me + p, n)).start()
        dst[me] = summed

    def gathered(which, dst):
        block = dst.at[pl.ds(0, n - 1)]
        copy_to(which * chunks, block, block, lax.rem(me + 1, n)).wait()
        return dst[...].astype(F32).reshape(c, dst.shape[2])

    cols[...] = params[...].T
    emb0, emb1 = cols[:, 0:1], cols[:, 1:2]
    g_on, g_om, g_in, g_im = (cols[:, q : q + 1] for q in range(2, 6))

    @pl.loop(0, chunks)
    def _(k):
        ds = lanes_of(k)
        same = masks[1:2, ds] > 0.5
        x = pair[ds, :].astype(F32).T + jnp.where(same, emb1, emb0)
        start[:, ds] = x
        hat, _ = norm_stats(x)
        nb = (hat * g_on).astype(BF16)
        normed[:, ds] = nb
        p = tn(out_proj[...], nb)
        pm = masks[0:1, ds]
        put(a_s, ds, pm * sigmoid(p[:c]) * p[c : 2 * c])
        put(b_s, ds, pm * sigmoid(p[2 * c : 3 * c]) * p[3 * c :])
        spread(B_OUT, b_s, b_r, k, ds)

    @pl.loop(0, chunks)
    def _(k):
        spread(A_OUT, a_s, a_r, k, lanes_of(k))

    @pl.loop(0, chunks)
    def _(k):
        ds = lanes_of(k)
        gate[:, ds] = sigmoid(tn(out_gate[...], normed[:, ds]))
        cot_t[:, ds] = cot[ds, :].astype(F32).T

    @pl.loop(0, chunks)
    def _(k):
        collect(B_OUT, b_s, b_r, k, lanes_of(k))
        to_slab(b_r, slab_b, k)

    for ch in range(per):
        mat_b[ch] = matrix(slab_b, ch)

    group = n * crows

    @pl.loop(0, chunks)
    def _(k):
        ds = lanes_of(k)
        collect(A_OUT, a_s, a_r, k, ds)
        to_slab(a_r, slab_a, k, True)
        for ch in range(per):
            keep(slab_o, ch, nt(matrix(slab_a, ch, k * group, group), mat_b[ch]), k * group)
        from_slab(slab_o, x_s, k, True)
        spread(X_OUT, x_s, x_r, k, ds)

    @pl.loop(0, chunks)
    def _(k):
        ds = lanes_of(k)
        collect(X_OUT, x_s, x_r, k, ds)
        hat, _ = norm_stats(take(x_r, ds))
        y = (hat * g_om).astype(BF16)
        m = (start[:, ds] + gate[:, ds] * tn(out_final[...], y)).astype(BF16)
        mid[:, ds] = m
        hat, _ = norm_stats(m.astype(F32))
        nb = (hat * g_in).astype(BF16)
        normed[:, ds] = nb
        p = tn(in_proj[...], nb)
        in_p[:, ds] = p
        pm = masks[0:1, ds]
        put(a2_s, ds, pm * sigmoid(p[:c]) * p[c : 2 * c])
        put(b2_s, ds, pm * sigmoid(p[2 * c : 3 * c]) * p[3 * c :])
        spread(A_IN, a2_s, a2_r, k, ds)
        spread(B_IN, b2_s, b2_r, k, ds)

    @pl.loop(0, chunks)
    def _(k):
        ds = lanes_of(k)
        s = sigmoid(tn(in_gate[...], normed[:, ds]))
        logit_s[:, ds] = s
        v = (cot_t[:, ds] * s).astype(BF16)
        gv[:, ds] = v
        gy[:, ds] = nn(in_final[...], v)

    acc_p[...] = jnp.zeros_like(acc_p)
    acc_g[...] = jnp.zeros_like(acc_g)
    acc_f[...] = jnp.zeros_like(acc_f)
    acc_n[...] = jnp.zeros_like(acc_n)
    acc_m[...] = jnp.zeros_like(acc_m)

    @pl.loop(0, chunks)
    def _(k):
        collect(A_IN, a2_s, a2_r, k, lanes_of(k))
        to_slab(a2_r, slab_a, k)
        collect(B_IN, b2_s, b2_r, k, lanes_of(k))
        to_slab(b2_r, slab_b, k)

    for ch in range(per):
        a = matrix(slab_a, ch)
        b = matrix(slab_b, ch)
        mat_a[ch] = a
        mat_b[ch] = b
        keep(slab_o, ch, tn(a, b))

    @pl.loop(0, chunks)
    def _(k):
        from_slab(slab_o, x2_s, k)
        spread(X_IN, x2_s, x2_r, k, lanes_of(k))

    @pl.loop(0, chunks)
    def _(k):
        ds = lanes_of(k)
        collect(X_IN, x2_s, x2_r, k, ds)
        hat, inv = norm_stats(take(x2_r, ds))
        y = (hat * g_im).astype(BF16)
        value = tn(in_final[...], y)
        s = logit_s[:, ds]
        grad_l = (cot_t[:, ds] * value * s * (1.0 - s)).astype(BF16)
        gl[:, ds] = grad_l
        g = gy[:, ds]
        acc_m[...] += lane_sum(g * hat)
        put(gx_s, ds, norm_back(g, hat, inv, g_im))
        spread(G_X, gx_s, gx_r, k, ds)
        acc_f[...] += nt(y, gv[:, ds])

    @pl.loop(0, chunks)
    def _(k):
        ds = lanes_of(k)
        grad_l = gl[:, ds]
        acc_g[...] += nt(normed[:, ds], grad_l)
        gy[:, ds] = nn(in_gate[...], grad_l)

    h_s[...] = early().reshape(n, per, 2 * c).astype(BF16)
    spread(H_SUM, h_s, h_r)

    @pl.loop(0, chunks)
    def _(k):
        collect(G_X, gx_s, gx_r, k, lanes_of(k))
        to_slab(gx_r, slab_a, k)

    for ch in range(per):
        gx = matrix(slab_a, ch)
        keep(slab_o, ch, nt(mat_b[ch], gx))
        keep(slab_p, ch, nn(mat_a[ch], gx))

    @pl.loop(0, chunks)
    def _(k):
        from_slab(slab_o, ga_s, k)
        spread(G_A, ga_s, ga_r, k, lanes_of(k))
        from_slab(slab_p, gb_s, k)
        spread(G_B, gb_s, gb_r, k, lanes_of(k))

    collect(H_SUM, h_s, h_r)
    hand_round(H_ALL, h_r, u_s, u_r)

    @pl.loop(0, chunks)
    def _(k):
        ds = lanes_of(k)
        collect(G_A, ga_s, ga_r, k, ds)
        collect(G_B, gb_s, gb_r, k, ds)
        pm = masks[0:1, ds]
        s0 = sigmoid(in_p[:c, ds])
        s2 = sigmoid(in_p[2 * c : 3 * c, ds])
        ga = take(ga_r, ds) * pm * s0
        gb = take(gb_r, ds) * pm * s2
        q0 = (ga * in_p[c : 2 * c, ds] * (1.0 - s0)).astype(BF16)
        q2 = (gb * in_p[3 * c :, ds] * (1.0 - s2)).astype(BF16)
        q = jnp.concatenate([q0, ga.astype(BF16), q2, gb.astype(BF16)], axis=0)
        acc_p[...] += nt(normed[:, ds], q)
        g = nn(in_proj[...], q) + gy[:, ds]
        hat, inv = norm_stats(mid[:, ds].astype(F32))
        acc_n[...] += lane_sum(g * hat)
        z = cot_t[:, ds] + norm_back(g, hat, inv, g_in)
        grad_out[ds, :] = z.T.astype(BF16)

    lane = lax.broadcasted_iota(jnp.int32, (c, LANES), 1)
    gains = jnp.where(lane == 0, acc_n[...], jnp.where(lane == 1, acc_m[...], 0.0))
    whole = jnp.concatenate([acc_p[...], gains], axis=1) * inv_count
    g_s[...] = whole.reshape(n, per, whole.shape[1]).astype(BF16)
    spread(P_SUM, g_s, g_r)
    both = gathered(H_ALL, u_r)
    gg_out[...] = both[:, :c]
    gf_out[...] = both[:, c:]
    collect(P_SUM, g_s, g_r)
    hand_round(P_ALL, g_r, t_s, t_r)
    final = gathered(P_ALL, t_r)
    gp_out[...] = final[:, : 4 * c]
    gains_out[...] = final[:, 4 * c :].T[:8]


def shards(n, pair, cotangent, residue_mask, chain_ids, chain_embed, out_norm_gain, out_proj,
           out_gate, out_mid_gain, out_final, in_norm_gain, in_proj, in_gate, in_mid_gain, in_final):
    rows, res, c = pair.shape
    total = rows * res
    per = c // n
    lc = res * min(
        q for q in range(1, rows + 1)
        if rows % q == 0 and q * res % LANES == 0 and (rows // q <= 3)
    )
    tiles = -(-res // LANES)
    row_start = lax.axis_index("dap") * rows
    row_mask = lax.dynamic_slice_in_dim(residue_mask, row_start, rows, 0)
    row_chain = lax.dynamic_slice_in_dim(chain_ids, row_start, rows, 0)
    pair_mask = (row_mask[:, None] * residue_mask[None, :]).astype(F32)
    same = (row_chain[:, None] == chain_ids[None, :]).astype(F32)
    masks = jnp.stack([pair_mask.reshape(total), same.reshape(total)])
    params = jnp.concatenate(
        [chain_embed, jnp.stack([out_norm_gain, out_mid_gain, in_norm_gain, in_mid_gain]),
         jnp.zeros((2, c), F32)], axis=0)

    def full(dtype):
        return pltpu.VMEM((c, total), dtype)

    swap = pltpu.VMEM((n, per, total), BF16)
    slab = pltpu.VMEM((tiles, res * per, LANES), F32)
    mats = pltpu.VMEM((per, res, res), BF16)
    wide = 4 * c + LANES
    scratch = [
        pltpu.VMEM((c, 8), F32), full(F32), full(BF16), full(F32),
        pltpu.VMEM((4 * c, total), F32), full(F32), full(BF16), full(F32), full(BF16), full(F32),
        full(BF16),
    ] + [swap] * 18 + [slab] * 4 + [mats] * 2 + [
        pltpu.VMEM((c, 4 * c), F32), pltpu.VMEM((c, c), F32), pltpu.VMEM((c, c), F32),
        pltpu.VMEM((c, 1), F32), pltpu.VMEM((c, 1), F32),
        pltpu.VMEM((n, per, wide), BF16), pltpu.VMEM((n, per, wide), BF16),
        pltpu.VMEM((per, wide), BF16), pltpu.VMEM((n, per, wide), BF16),
        pltpu.VMEM((n, per, 2 * c), BF16), pltpu.VMEM((n, per, 2 * c), BF16),
        pltpu.VMEM((per, 2 * c), BF16), pltpu.VMEM((n, per, 2 * c), BF16),
        pltpu.SemaphoreType.DMA((13 * (total // lc),)), pltpu.SemaphoreType.DMA((13 * (total // lc),)),
    ]
    vmem = pl.BlockSpec(memory_space=pltpu.VMEM)
    grad, gp, gg, gf, gains = pl.pallas_call(
        functools.partial(kernel, n, rows, res, lc),
        out_shape=(
            jax.ShapeDtypeStruct((total, c), BF16),
            jax.ShapeDtypeStruct((c, 4 * c), F32),
            jax.ShapeDtypeStruct((c, c), F32),
            jax.ShapeDtypeStruct((c, c), F32),
            jax.ShapeDtypeStruct((8, c), F32),
        ),
        in_specs=[vmem] * 10,
        out_specs=(vmem,) * 5,
        scratch_shapes=scratch,
        compiler_params=pltpu.CompilerParams(
            collective_id=0, has_side_effects=True, vmem_limit_bytes=60 * 1024 * 1024
        ),
    )(
        pair.reshape(total, c), cotangent.reshape(total, c), masks, params,
        out_proj, out_gate, out_final, in_proj, in_gate, in_final,
    )
    return grad.reshape(rows, res, c), gp, gg, gf, gains[0], gains[1]


def solution(mesh):
    split = P("dap", "cplx", None)
    return jax.shard_map(
        functools.partial(shards, mesh.shape["dap"]),
        mesh=mesh,
        in_specs=(split, split, P("cplx"), P("cplx")) + (P(),) * 11,
        out_specs=(split, P("cplx", None), P("cplx", None), P("cplx", None), P("cplx"), P("cplx")),
        check_vma=False,
    )
```

```python
import functools

import jax
import jax.numpy as jnp
from jax import lax
from jax.experimental import pallas as pl
from jax.experimental.pallas import tpu as pltpu
from jax.sharding import PartitionSpec as P

F32 = jnp.float32
BF16 = jnp.bfloat16
LANES = 128
A_OUT, B_OUT, X_OUT, A_IN, B_IN, X_IN, G_X, G_A, G_B, P_SUM, P_ALL, H_SUM, H_ALL, GAINS = range(14)


def tn(w, x):
    return lax.dot_general(w, x, (((0,), (0,)), ((), ())), preferred_element_type=F32)


def nn(w, x):
    return jnp.dot(w, x, preferred_element_type=F32)


def nt(w, x):
    return lax.dot_general(w, x, (((1,), (1,)), ((), ())), preferred_element_type=F32)


def sigmoid(v):
    return 1.0 / (1.0 + jnp.exp(-v))


def norm_stats(v):
    centred = v - jnp.mean(v, axis=0, keepdims=True)
    inv = lax.rsqrt(jnp.mean(centred * centred, axis=0, keepdims=True) + 1e-05)
    return centred * inv, inv


def norm_back(grad, hat, inv, gain):
    scaled = grad * gain
    m1 = jnp.mean(scaled, axis=0, keepdims=True)
    m2 = jnp.mean(scaled * hat, axis=0, keepdims=True)
    return inv * (scaled - m1 - hat * m2)


def lane_sum(v):
    return jnp.sum(v, axis=1, keepdims=True)


def kernel(
    n, rows, res, lc,
    pair, cot, residues, chains, embed, gain_on, gain_om, gain_in, gain_im, out_proj, out_gate, out_final, in_proj, in_gate, in_final,
    grad_out, gp_out, gg_out, gf_out, gn_out, gm_out,
    cols, masks, in_q, start, normed, gate, in_p, cot_t, mid, logit_s, gv, gy, gl,
    a_s, b_s, x_s, a_r, b_r, x_r,
    a2_s, b2_s, x2_s, a2_r, b2_r, x2_r,
    gx_s, gx_r, ga_s, gb_s, ga_r, gb_r,
    slab_a, slab_b, slab_o, slab_p, mat_a, mat_b, mat_x,
    acc_p, acc_g, acc_f, acc_n, acc_m, g_s, g_r, t_s, t_r, h_s, h_r, u_s, u_r, w_s, w_r,
    send_sem, recv_sem,
):
    me = lax.axis_index("dap")
    c = start.shape[0]
    per = c // n
    total = rows * res
    chunks = total // lc
    crows = lc // res
    tiles = -(-res // LANES)
    inv_count = 1.0 / res

    barrier = pltpu.get_barrier_semaphore()
    for p in range(1, n):
        pl.semaphore_signal(
            barrier, inc=1, device_id={"dap": lax.rem(me + p, n)},
            device_id_type=pl.DeviceIdType.MESH,
        )

    def copy_to(sem, src, dst, peer):
        return pltpu.make_async_remote_copy(
            src_ref=src, dst_ref=dst, send_sem=send_sem.at[sem], recv_sem=recv_sem.at[sem],
            device_id={"dap": peer}, device_id_type=pl.DeviceIdType.MESH,
        )

    def spread(which, src, dst, k=0, ds=None):
        def view(ref, at):
            return ref.at[at] if ds is None else ref.at[at, :, ds]

        for p in range(1, n):
            peer = lax.rem(me + p, n)
            copy_to(which * chunks + k, view(src, peer), view(dst, me), peer).start()
        if ds is None:
            dst[me] = src[me]
        else:
            dst[me, :, ds] = src[me, :, ds]

    def collect(which, src, dst, k=0, ds=None):
        def view(ref):
            return ref.at[pl.ds(0, n - 1)] if ds is None else ref.at[pl.ds(0, n - 1), :, ds]

        copy_to(which * chunks + k, view(src), view(dst), lax.rem(me + 1, n)).wait()

    def lanes_of(k):
        return pl.ds(pl.multiple_of(k * lc, lc), lc)

    def put(ref, ds, value):
        ref[:, :, ds] = value.reshape(n, per, lc).astype(BF16)

    def take(ref, ds):
        return ref[:, :, ds].astype(F32).reshape(c, lc)

    def to_slab(ref, slab, k, by_chunk=False):
        for s in range(n):
            block = ref[s, :, lanes_of(k)].astype(F32)
            row = (k * n + s) * crows if by_chunk else s * rows + k * crows
            for i in range(crows):
                part = block[:, i * res : (i + 1) * res]
                at = pl.ds(pl.multiple_of((row + i) * per, per), per)
                for t in range(tiles):
                    width = min(LANES, res - t * LANES)
                    slab[t, at, :width] = part[:, t * LANES : t * LANES + width]

    def matrix(slab, ch, first=0, count=res):
        at = pl.ds(first * per + ch, count, stride=per)
        parts = [slab[t, at, :] for t in range(tiles)]
        whole = parts[0] if tiles == 1 else jnp.concatenate(parts, axis=1)
        return whole[:, :res].astype(BF16)

    def keep(slab, ch, value, first=0):
        count = value.shape[0]
        pad = tiles * LANES - res
        if pad:
            value = jnp.concatenate([value, jnp.zeros((count, pad), F32)], axis=1)
        for t in range(tiles):
            at = pl.ds(first * per + ch, count, stride=per)
            slab[t, at, :] = value[:, t * LANES : (t + 1) * LANES]

    def from_slab(slab, ref, k, by_chunk=False):
        for s in range(n):
            row = (k * n + s) * crows if by_chunk else s * rows + k * crows
            parts = []
            for i in range(crows):
                at = pl.ds(pl.multiple_of((row + i) * per, per), per)
                for t in range(tiles):
                    width = min(LANES, res - t * LANES)
                    parts.append(slab[t, at, :width])
            ref[s, :, lanes_of(k)] = jnp.concatenate(parts, axis=1).astype(BF16)

    def early():
        return jnp.concatenate([acc_g[...], acc_f[...]], axis=1) * inv_count

    def hand_round(which, src, mine, dst):
        summed = jnp.sum(src[...].astype(F32), axis=0).astype(BF16)
        mine[...] = summed
        for p in range(1, n):
            copy_to(which * chunks, mine, dst.at[me], lax.rem(me + p, n)).start()
        dst[me] = summed

    def gathered(which, dst):
        block = dst.at[pl.ds(0, n - 1)]
        copy_to(which * chunks, block, block, lax.rem(me + 1, n)).wait()
        return dst[...].astype(F32).reshape(c, dst.shape[2])

    params = [embed[...], gain_on[...], gain_om[...], gain_in[...], gain_im[...]]
    cols[...] = jnp.concatenate(params + [jnp.zeros((2, c), F32)], axis=0).T
    here = lax.broadcasted_iota(jnp.int32, (rows, res), 1) == (
        lax.broadcasted_iota(jnp.int32, (rows, res), 0) + me * rows
    )
    row_mask = jnp.sum(jnp.where(here, residues[...], 0).astype(F32), axis=1, keepdims=True)
    row_chain = jnp.sum(jnp.where(here, chains[...], 0).astype(F32), axis=1, keepdims=True)
    both = row_mask * residues[...].astype(F32)
    same_chain = jnp.where(row_chain == chains[...].astype(F32), 1.0, 0.0)
    masks[0:1, :] = jnp.concatenate([both[i : i + 1] for i in range(rows)], axis=1)
    masks[1:2, :] = jnp.concatenate([same_chain[i : i + 1] for i in range(rows)], axis=1)
    emb0, emb1 = cols[:, 0:1], cols[:, 1:2]
    g_on, g_om, g_in, g_im = (cols[:, q : q + 1] for q in range(2, 6))

    def project(k):
        ds = lanes_of(k)
        same = masks[1:2, ds] > 0.5
        x = pair[ds, :].astype(F32).T + jnp.where(same, emb1, emb0)
        start[:, ds] = x
        hat, _ = norm_stats(x)
        nb = (hat * g_on).astype(BF16)
        normed[:, ds] = nb
        p = tn(out_proj[...], nb)
        pm = masks[0:1, ds]
        put(a_s, ds, pm * sigmoid(p[:c]) * p[c : 2 * c])
        put(b_s, ds, pm * sigmoid(p[2 * c : 3 * c]) * p[3 * c :])

    project(0)
    pl.semaphore_wait(barrier, n - 1)
    spread(B_OUT, b_s, b_r, 0, lanes_of(0))

    @pl.loop(1, chunks)
    def _(k):
        project(k)
        spread(B_OUT, b_s, b_r, k, lanes_of(k))

    @pl.loop(0, chunks)
    def _(k):
        spread(A_OUT, a_s, a_r, k, lanes_of(k))

    @pl.loop(0, chunks)
    def _(k):
        ds = lanes_of(k)
        gate[:, ds] = sigmoid(tn(out_gate[...], normed[:, ds]))
        cot_t[:, ds] = cot[ds, :].astype(F32).T

    @pl.loop(0, chunks)
    def _(k):
        collect(B_OUT, b_s, b_r, k, lanes_of(k))
        to_slab(b_r, slab_b, k)

    for ch in range(per):
        mat_b[ch] = matrix(slab_b, ch)

    group = n * crows

    @pl.loop(0, chunks)
    def _(k):
        ds = lanes_of(k)
        collect(A_OUT, a_s, a_r, k, ds)
        to_slab(a_r, slab_a, k, True)
        for ch in range(per):
            keep(slab_o, ch, nt(matrix(slab_a, ch, k * group, group), mat_b[ch]), k * group)
        from_slab(slab_o, x_s, k, True)
        spread(X_OUT, x_s, x_r, k, ds)

    @pl.loop(0, chunks)
    def _(k):
        ds = lanes_of(k)
        collect(X_OUT, x_s, x_r, k, ds)
        hat, _ = norm_stats(take(x_r, ds))
        y = (hat * g_om).astype(BF16)
        m = (start[:, ds] + gate[:, ds] * tn(out_final[...], y)).astype(BF16)
        mid[:, ds] = m
        hat, _ = norm_stats(m.astype(F32))
        nb = (hat * g_in).astype(BF16)
        normed[:, ds] = nb
        p = tn(in_proj[...], nb)
        in_p[:, ds] = p
        pm = masks[0:1, ds]
        put(a2_s, ds, pm * sigmoid(p[:c]) * p[c : 2 * c])
        put(b2_s, ds, pm * sigmoid(p[2 * c : 3 * c]) * p[3 * c :])
        spread(A_IN, a2_s, a2_r, k, ds)
        spread(B_IN, b2_s, b2_r, k, ds)

    @pl.loop(0, chunks)
    def _(k):
        ds = lanes_of(k)
        s = sigmoid(tn(in_gate[...], normed[:, ds]))
        logit_s[:, ds] = s
        v = (cot_t[:, ds] * s).astype(BF16)
        gv[:, ds] = v
        gy[:, ds] = nn(in_final[...], v)

    acc_p[...] = jnp.zeros_like(acc_p)
    acc_g[...] = jnp.zeros_like(acc_g)
    acc_f[...] = jnp.zeros_like(acc_f)
    acc_n[...] = jnp.zeros_like(acc_n)
    acc_m[...] = jnp.zeros_like(acc_m)

    @pl.loop(0, chunks)
    def _(k):
        collect(A_IN, a2_s, a2_r, k, lanes_of(k))
        to_slab(a2_r, slab_a, k)
        collect(B_IN, b2_s, b2_r, k, lanes_of(k))
        to_slab(b2_r, slab_b, k)

    for ch in range(per):
        a = matrix(slab_a, ch)
        b = matrix(slab_b, ch)
        mat_a[ch] = a
        mat_b[ch] = b
        keep(slab_o, ch, tn(a, b))

    @pl.loop(0, chunks)
    def _(k):
        from_slab(slab_o, x2_s, k)
        spread(X_IN, x2_s, x2_r, k, lanes_of(k))

    @pl.loop(0, chunks)
    def _(k):
        ds = lanes_of(k)
        collect(X_IN, x2_s, x2_r, k, ds)
        hat, inv = norm_stats(take(x2_r, ds))
        y = (hat * g_im).astype(BF16)
        value = tn(in_final[...], y)
        s = logit_s[:, ds]
        grad_l = (cot_t[:, ds] * value * s * (1.0 - s)).astype(BF16)
        gl[:, ds] = grad_l
        g = gy[:, ds]
        acc_m[...] += lane_sum(g * hat)
        put(gx_s, ds, norm_back(g, hat, inv, g_im))
        spread(G_X, gx_s, gx_r, k, ds)
        acc_f[...] += nt(y, gv[:, ds])

    @pl.loop(0, chunks)
    def _(k):
        ds = lanes_of(k)
        grad_l = gl[:, ds]
        acc_g[...] += nt(normed[:, ds], grad_l)
        gy[:, ds] = nn(in_gate[...], grad_l)

    h_s[...] = early().reshape(n, per, 2 * c).astype(BF16)
    spread(H_SUM, h_s, h_r)

    @pl.loop(0, chunks)
    def _(k):
        collect(G_X, gx_s, gx_r, k, lanes_of(k))
        to_slab(gx_r, slab_a, k)

    for ch in range(per):
        gx = matrix(slab_a, ch)
        mat_x[ch] = gx
        keep(slab_o, ch, nt(mat_b[ch], gx))

    @pl.loop(0, chunks)
    def _(k):
        from_slab(slab_o, ga_s, k)
        spread(G_A, ga_s, ga_r, k, lanes_of(k))

    for ch in range(per):
        keep(slab_p, ch, nn(mat_a[ch], mat_x[ch]))

    @pl.loop(0, chunks)
    def _(k):
        from_slab(slab_p, gb_s, k)
        spread(G_B, gb_s, gb_r, k, lanes_of(k))

    collect(H_SUM, h_s, h_r)
    hand_round(H_ALL, h_r, u_s, u_r)

    @pl.loop(0, chunks)
    def _(k):
        ds = lanes_of(k)
        collect(G_A, ga_s, ga_r, k, ds)
        collect(G_B, gb_s, gb_r, k, ds)
        pm = masks[0:1, ds]
        s0 = sigmoid(in_p[:c, ds])
        s2 = sigmoid(in_p[2 * c : 3 * c, ds])
        ga = take(ga_r, ds) * pm * s0
        gb = take(gb_r, ds) * pm * s2
        q0 = (ga * in_p[c : 2 * c, ds] * (1.0 - s0)).astype(BF16)
        q2 = (gb * in_p[3 * c :, ds] * (1.0 - s2)).astype(BF16)
        q = jnp.concatenate([q0, ga.astype(BF16), q2, gb.astype(BF16)], axis=0)
        in_q[:, ds] = q
        acc_p[...] += nt(normed[:, ds], q)

    g_s[...] = (acc_p[...] * inv_count).reshape(n, per, 4 * c).astype(BF16)
    spread(P_SUM, g_s, g_r)

    @pl.loop(0, chunks)
    def _(k):
        ds = lanes_of(k)
        g = nn(in_proj[...], in_q[:, ds]) + gy[:, ds]
        hat, inv = norm_stats(mid[:, ds].astype(F32))
        acc_n[...] += lane_sum(g * hat)
        z = cot_t[:, ds] + norm_back(g, hat, inv, g_in)
        grad_out[ds, :] = z.T.astype(BF16)

    lane = lax.broadcasted_iota(jnp.int32, (c, LANES), 1)
    gains = jnp.where(lane == 0, acc_n[...], jnp.where(lane == 1, acc_m[...], 0.0))
    w_s[...] = (gains * inv_count).T[:8]
    for p in range(1, n):
        copy_to(GAINS * chunks, w_s, w_r.at[me], lax.rem(me + p, n)).start()
    w_r[me] = w_s[...]
    collect(P_SUM, g_s, g_r)
    hand_round(P_ALL, g_r, t_s, t_r)
    both = gathered(H_ALL, u_r)
    gg_out[...] = both[:, :c]
    gf_out[...] = both[:, c:]
    block = w_r.at[pl.ds(0, n - 1)]
    copy_to(GAINS * chunks, block, block, lax.rem(me + 1, n)).wait()
    gain_sums = jnp.sum(w_r[...], axis=0)
    gn_out[...] = gain_sums[0:1]
    gm_out[...] = gain_sums[1:2]
    gp_out[...] = gathered(P_ALL, t_r)


def shards(n, pair, cotangent, residue_mask, chain_ids, chain_embed, out_norm_gain, out_proj,
           out_gate, out_mid_gain, out_final, in_norm_gain, in_proj, in_gate, in_mid_gain, in_final):
    rows, res, c = pair.shape
    total = rows * res
    per = c // n
    lc = res * min(
        q for q in range(1, rows + 1)
        if rows % q == 0 and q * res % LANES == 0 and (rows // q <= 3)
    )
    tiles = -(-res // LANES)
    def full(dtype):
        return pltpu.VMEM((c, total), dtype)

    swap = pltpu.VMEM((n, per, total), BF16)
    slab = pltpu.VMEM((tiles, res * per, LANES), F32)
    mats = pltpu.VMEM((per, res, res), BF16)
    wide = 4 * c
    scratch = [
        pltpu.VMEM((c, 8), F32), pltpu.VMEM((2, total), F32), pltpu.VMEM((4 * c, total), BF16), full(F32), full(BF16), full(F32),
        pltpu.VMEM((4 * c, total), F32), full(F32), full(BF16), full(F32), full(BF16), full(F32),
        full(BF16),
    ] + [swap] * 18 + [slab] * 4 + [mats] * 3 + [
        pltpu.VMEM((c, 4 * c), F32), pltpu.VMEM((c, c), F32), pltpu.VMEM((c, c), F32),
        pltpu.VMEM((c, 1), F32), pltpu.VMEM((c, 1), F32),
        pltpu.VMEM((n, per, wide), BF16), pltpu.VMEM((n, per, wide), BF16),
        pltpu.VMEM((per, wide), BF16), pltpu.VMEM((n, per, wide), BF16),
        pltpu.VMEM((n, per, 2 * c), BF16), pltpu.VMEM((n, per, 2 * c), BF16),
        pltpu.VMEM((per, 2 * c), BF16), pltpu.VMEM((n, per, 2 * c), BF16),
        pltpu.VMEM((8, c), F32), pltpu.VMEM((n, 8, c), F32),
        pltpu.SemaphoreType.DMA((14 * (total // lc),)), pltpu.SemaphoreType.DMA((14 * (total // lc),)),
    ]
    vmem = pl.BlockSpec(memory_space=pltpu.VMEM)
    grad, gp, gg, gf, gn, gm = pl.pallas_call(
        functools.partial(kernel, n, rows, res, lc),
        out_shape=(
            jax.ShapeDtypeStruct((total, c), BF16),
            jax.ShapeDtypeStruct((c, 4 * c), F32),
            jax.ShapeDtypeStruct((c, c), F32),
            jax.ShapeDtypeStruct((c, c), F32),
            jax.ShapeDtypeStruct((1, c), F32),
            jax.ShapeDtypeStruct((1, c), F32),
        ),
        in_specs=[vmem] * 15,
        out_specs=(vmem,) * 6,
        scratch_shapes=scratch,
        compiler_params=pltpu.CompilerParams(
            collective_id=0, has_side_effects=True, vmem_limit_bytes=60 * 1024 * 1024
        ),
    )(
        pair.reshape(total, c), cotangent.reshape(total, c),
        residue_mask.reshape(1, res), chain_ids.reshape(1, res), chain_embed,
        out_norm_gain.reshape(1, c), out_mid_gain.reshape(1, c),
        in_norm_gain.reshape(1, c), in_mid_gain.reshape(1, c),
        out_proj, out_gate, out_final, in_proj, in_gate, in_final,
    )
    return grad.reshape(rows, res, c), gp, gg, gf, gn.reshape(c), gm.reshape(c)


def solution(mesh):
    split = P("dap", "cplx", None)
    return jax.shard_map(
        functools.partial(shards, mesh.shape["dap"]),
        mesh=mesh,
        in_specs=(split, split, P("cplx"), P("cplx")) + (P(),) * 11,
        out_specs=(split, P("cplx", None), P("cplx", None), P("cplx", None), P("cplx"), P("cplx")),
        check_vma=False,
    )
```
